32 devices in a mesh: expert: 4 (over z), shard: 8 (over y, x, core).
Axes of the slice: x: 2, y: 2, z: 4, core: 2. Of those that a mesh axis runs over, the one named last changes fastest.
Arguments:
- tokens: bfloat16 [768, 4096], P(('expert', 'shard')), may hold values from -0.19921875 to 0.19921875
- expert_ids: int32 [768, 2], P(('expert', 'shard')), may hold values from 0 to 3, all different within a row; in each aligned block of 24 rows (0 to 23, 24 to 47, ...) at most 16 rows name the same one
- weight_gate: bfloat16 [4, 4096, 8192], P('expert', None, 'shard'), may hold values from -0.09375 to 0.09375
- weight_up: bfloat16 [4, 4096, 8192], P('expert', None, 'shard'), may hold values from -0.09375 to 0.09375
- gate_pre: bfloat16 [4, 512, 8192], P('expert', None, 'shard'), may hold values from -8 to 8
- up_pre: bfloat16 [4, 512, 8192], P('expert', None, 'shard'), may hold values from -6 to 6
- hidden_grad: bfloat16 [4, 512, 8192], P('expert', None, 'shard'), may hold values from -6 to 6
Outputs:
- token_grad: bfloat16 [768, 4096], P(('expert', 'shard'))
- gate_weight_grad: float32 [4, 4096, 8192], P('expert', None, 'shard')
- up_weight_grad: float32 [4, 4096, 8192], P('expert', None, 'shard')
The draws below stay inside these ranges and needn't reach their ends.
Inputs may be any that keep to these rules, and one draw needn't show every extreme that they name: `expert_ids`: each token names 2 different experts. Among the tokens of one device no expert is named more than 16 times, and in every draw some device names some expert exactly 16 times.
All inputs are finite; a program needn't handle non-finite values.
Results may differ from the reference program's by a relative error of at most 0.02.
Values may be sent and summed in bfloat16 or wider, within the bound.
A program may use at most 192 MiB of HBM per device.

```python
import math
import jax
import jax.numpy as jnp
import numpy as np
from jax import lax

D = 4096
FF = 8192
TOP = 2
TOK_DEV = 24
CAP = 16
EXPERTS = 4
TOKENS = 768
GROUP_ROWS = 512
N_EXPERT = 4
N_SHARD = 8


def shard_levels(rng, dims, split, smallest, high):
    loudness = 1.0
    for dim, shards_of in split:
        steps = jax.random.uniform(jax.random.fold_in(jax.random.fold_in(rng, 6), dim), (shards_of,), jnp.float32, smallest / len(split), high / len(split))
        loudness = loudness * jnp.repeat(jnp.exp(steps), dims[dim] // shards_of).reshape((-1,) + (1,) * (len(dims) - 1 - dim))
    return loudness


def shared_out(own_key, own, number, rows, amount, top, bound, slope):
    sequence = jax.random.permutation(own_key, amount)
    heavy_load, ordinary = load_shares(amount, rows * top, bound, slope, True), load_shares(amount, rows * top, bound, slope, False)
    places = jnp.arange(amount)

    def named(tallies, turn):
        used = int((tallies > 0).sum())
        fixed = max(1, used // 4)
        moved = fixed + (places - fixed + turn * (used - fixed)) % max(1, amount - fixed)
        return jnp.zeros((amount,), jnp.int32).at[sequence[jnp.where(places < fixed, places, moved)]].set(jnp.asarray(tallies, jnp.int32))

    tallies = jnp.where(number % 4 == 0, named(heavy_load, number // 4), named(ordinary, number - number // 4 - 1))
    mixed = jax.random.permutation(jax.random.fold_in(own, 3), amount)
    source_of, receiver = mixed[0:amount // 2 * 2:2], mixed[1:amount // 2 * 2:2]
    slack = jnp.minimum(tallies[source_of] - 1, bound - tallies[receiver]) // 2
    slack = jnp.where((source_of == sequence[0]) | (receiver == sequence[0]) | (tallies[receiver] == 0), 0, jnp.maximum(slack, 0))
    moved = jax.random.randint(jax.random.fold_in(own, 4), (amount // 2,), 0, 1 << 20) % (slack + 1)
    tallies = tallies.at[source_of].add(-moved).at[receiver].add(moved)
    items = jnp.searchsorted(jnp.cumsum(tallies), jnp.arange(rows * top), side="right").astype(jnp.int32)
    listing = items.reshape(top, rows).T
    listing = listing[jax.random.permutation(jax.random.fold_in(own, 1), rows)]
    turn = jax.random.randint(jax.random.fold_in(own, 2), (rows, 1), 0, top)
    return jnp.take_along_axis(listing, (jnp.arange(top)[None, :] + turn) % top, axis=1)


def load_shares(number_of, total, limit, skew, full):
    portions = [(1 << 20) // math.isqrt(standing ** skew) + 1 for standing in range(1, number_of + 1)]
    largest = limit if full else min(limit, max(-(-total // number_of), total * portions[0] // sum(portions)))
    least = 1 if total - largest >= number_of - 1 else 0
    given, surplus = [largest] + [least] * (number_of - 1), total - largest - least * (number_of - 1)
    while surplus > 0:
        free = [i for i in range(1, number_of) if given[i] < largest] or [i for i in range(1, number_of) if given[i] < limit]
        whole, budget = sum([portions[i] for i in free]), surplus
        for i in free:
            addition = min(limit - given[i], max(1, budget * portions[i] // whole), surplus)
            given[i] = given[i] + addition
            surplus = surplus - addition
    return np.array(given)


def centred(key, extent, spread, bound, pieces=(), held_as=jnp.bfloat16):
    gain = shard_levels(key, extent, pieces, -0.22, 0.18) if pieces else 1.0
    drawn = jax.random.normal(key, extent, jnp.float32) * spread * gain
    return jnp.minimum(jnp.maximum(drawn, -bound), bound).astype(held_as)


def setup_inputs(seed: int = 0) -> dict:
    streams_of = jax.random.split(jax.random.key(seed), 8)
    tokens = centred(streams_of[0], (TOKENS, D), 0.03, 0.19921875, ((0, 32),))
    expert_ids_keys = jax.random.split(jax.random.fold_in(streams_of[1], 1), TOKENS // TOK_DEV)
    expert_ids_turns = jax.random.permutation(jax.random.fold_in(streams_of[1], 3), TOKENS // TOK_DEV)
    expert_ids = jax.vmap(lambda own, number: shared_out(jax.random.fold_in(streams_of[1], 2), own, number, TOK_DEV, EXPERTS, TOP, CAP, 2))(expert_ids_keys, expert_ids_turns).reshape((TOKENS, TOP))
    weight_gate = centred(streams_of[2], (EXPERTS, D, FF), D ** -0.5, 0.09375, ((0, 4), (2, 8)))
    weight_up = centred(streams_of[3], (EXPERTS, D, FF), D ** -0.5, 0.09375, ((0, 4), (2, 8)))
    gate_pre = centred(streams_of[4], (EXPERTS, GROUP_ROWS, FF), 1.5, 8.0, ((0, 4), (2, 8)))
    up_pre = centred(streams_of[5], (EXPERTS, GROUP_ROWS, FF), 1.0, 6.0, ((0, 4), (2, 8)))
    hidden_grad = centred(streams_of[6], (EXPERTS, GROUP_ROWS, FF), 1.0, 6.0, ((0, 4), (2, 8)))
    return {"tokens": tokens, "expert_ids": expert_ids, "weight_gate": weight_gate, "weight_up": weight_up, "gate_pre": gate_pre, "up_pre": up_pre, "hidden_grad": hidden_grad}


def swiglu_grads(gate_values, up_values, hidden_cotangent):
    gate_float = gate_values.astype(jnp.float32)
    up_float = up_values.astype(jnp.float32)
    cotangent = hidden_cotangent.astype(jnp.float32)
    sigmoid_gate = jax.nn.sigmoid(gate_float)
    gate_grad = (cotangent * up_float * sigmoid_gate * (1.0 + gate_float * (1.0 - sigmoid_gate))).astype(jnp.bfloat16)
    up_grad = (cotangent * gate_float * sigmoid_gate).astype(jnp.bfloat16)
    return gate_grad, up_grad


def reference(tokens, expert_ids, weight_gate, weight_up, gate_pre, up_pre, hidden_grad):
    devices_all = N_EXPERT * N_SHARD
    width = tokens.shape[1]
    labels = jnp.arange(N_EXPERT, dtype=jnp.int32)
    one_hot = (expert_ids[:, :, None] == labels[None, None, :]).astype(jnp.int32)
    per_device = one_hot.reshape(devices_all, TOK_DEV * TOP, N_EXPERT)
    earlier = jnp.cumsum(per_device, axis=1) - per_device
    slot_index = jnp.sum(per_device * earlier, axis=2).reshape(TOKENS, TOP).astype(jnp.int32)
    token_index = jnp.arange(TOKENS, dtype=jnp.int32)
    device_index = token_index // TOK_DEV
    source_group = device_index // N_SHARD
    source_shard = device_index % N_SHARD
    row_index = ((source_shard * N_EXPERT + source_group)[:, None] * CAP + slot_index).astype(jnp.int32)
    dispatched = jnp.zeros((N_EXPERT, GROUP_ROWS, width), jnp.bfloat16)
    copies = jnp.broadcast_to(tokens[:, None, :], (TOKENS, TOP, width))
    dispatched = dispatched.at[expert_ids, row_index].set(copies)
    block_width = FF // N_SHARD
    gate_wgrads = []
    up_wgrads = []
    slot_grads = []
    for expert in range(N_EXPERT):
        gate_grad, up_grad = swiglu_grads(gate_pre[expert], up_pre[expert], hidden_grad[expert])
        rows_here = dispatched[expert]
        gate_wgrads.append(jnp.dot(rows_here.T, gate_grad, preferred_element_type=jnp.float32))
        up_wgrads.append(jnp.dot(rows_here.T, up_grad, preferred_element_type=jnp.float32))
        gate_matrix = weight_gate[expert]
        up_matrix = weight_up[expert]

        def add_block(total, block_number):
            first_unit = (block_number * block_width).astype(jnp.int32)
            gate_block = lax.dynamic_slice_in_dim(gate_grad, first_unit, block_width, 1)
            up_block = lax.dynamic_slice_in_dim(up_grad, first_unit, block_width, 1)
            gate_weights = lax.dynamic_slice_in_dim(gate_matrix, first_unit, block_width, 1)
            up_weights = lax.dynamic_slice_in_dim(up_matrix, first_unit, block_width, 1)
            block_term = jnp.dot(gate_block, gate_weights.T, preferred_element_type=jnp.float32)
            block_term = block_term + jnp.dot(up_block, up_weights.T, preferred_element_type=jnp.float32)
            return total + block_term.astype(jnp.bfloat16).astype(jnp.float32), None

        start_total = jnp.zeros((GROUP_ROWS, width), jnp.float32)
        total, unused = lax.scan(add_block, start_total, jnp.arange(N_SHARD, dtype=jnp.int32))
        slot_grads.append(total.astype(jnp.bfloat16))
    slot_all = jnp.stack(slot_grads)
    picked = slot_all[expert_ids, row_index].astype(jnp.float32)
    token_grad = jnp.sum(picked, axis=1).astype(jnp.bfloat16)
    return token_grad, jnp.stack(gate_wgrads), jnp.stack(up_wgrads)
```

```python
import functools
import jax
import jax.numpy as jnp
from jax import lax
from jax.experimental import pallas as pl
from jax.experimental.pallas import tpu as pltpu
from jax.sharding import PartitionSpec as P

MESH = pl.DeviceIdType.MESH
CHUNKS = 8
COPIES = 21


def swiglu_grads(gate_values, up_values, hidden_cotangent):
    gate_float = gate_values.astype(jnp.float32)
    up_float = up_values.astype(jnp.float32)
    cotangent = hidden_cotangent.astype(jnp.float32)
    sigmoid_gate = jax.nn.sigmoid(gate_float)
    gate_grad = (
        cotangent * up_float * sigmoid_gate * (1.0 + gate_float * (1.0 - sigmoid_gate))
    ).astype(jnp.bfloat16)
    up_grad = (cotangent * gate_float * sigmoid_gate).astype(jnp.bfloat16)
    return (gate_grad, up_grad)


def slot_table(expert_ids, groups, capacity):
    token_count = expert_ids.shape[0]
    choices_per = expert_ids.shape[1]
    labels = lax.broadcasted_iota(jnp.int32, (1, 1, groups), 2)
    one_hot = (expert_ids[:, :, None] == labels).astype(jnp.int32)
    flat_hits = one_hot.reshape(token_count * choices_per, groups)
    earlier = jnp.cumsum(flat_hits, axis=0) - flat_hits
    slot_index = jnp.sum(flat_hits * earlier, axis=1).reshape(token_count, choices_per)
    slot_labels = lax.broadcasted_iota(jnp.int32, (1, 1, 1, capacity), 3)
    slot_hits = one_hot[:, :, :, None] * (slot_index[:, :, None, None] == slot_labels).astype(
        jnp.int32
    )
    selection = jnp.sum(slot_hits, axis=1).reshape(token_count, groups * capacity)
    return selection.astype(jnp.bfloat16)


def rows_inner(left_rows, right_rows):
    return lax.dot_general(
        left_rows, right_rows, (((0,), (0,)), ((), ())), preferred_element_type=jnp.float32
    )


def times_transposed(left_rows, weights):
    return lax.dot_general(
        left_rows, weights, (((1,), (1,)), ((), ())), preferred_element_type=jnp.float32
    )


def on_device_general(tokens, expert_ids, weight_gate, weight_up, gate_pre, up_pre, hidden_grad):
    groups = lax.axis_size("expert")
    shards = lax.axis_size("shard")
    model_width = tokens.shape[1]
    capacity = gate_pre.shape[1] // (groups * shards)
    selection = slot_table(expert_ids, groups, capacity)
    outgoing = rows_inner(selection, tokens).astype(jnp.bfloat16)
    gate_grad, up_grad = swiglu_grads(gate_pre[0], up_pre[0], hidden_grad[0])
    gate_matrix = weight_gate[0]
    up_matrix = weight_up[0]
    arrived = lax.all_to_all(
        outgoing.reshape(groups, capacity, model_width),
        "expert",
        split_axis=0,
        concat_axis=0,
        tiled=True,
    )
    block_rows = lax.all_gather(
        arrived.reshape(groups * capacity, model_width), "shard", axis=0, tiled=True
    )
    gate_rows = gate_grad
    up_rows = up_grad
    gate_wgrad = rows_inner(block_rows, gate_rows)
    up_wgrad = rows_inner(block_rows, up_rows)
    gate_rows = gate_grad
    up_rows = up_grad
    summed = lax.psum_scatter(
        (times_transposed(gate_rows, gate_matrix) + times_transposed(up_rows, up_matrix)).astype(
            jnp.bfloat16
        ),
        "shard",
        scatter_dimension=0,
        tiled=True,
    )
    outbound = summed.reshape(groups, capacity, model_width)
    returned = lax.all_to_all(outbound, "expert", split_axis=0, concat_axis=0, tiled=True)
    returned = returned.reshape(groups * capacity, model_width)
    token_grad = times_transposed(selection, returned.T).astype(jnp.bfloat16)
    return (token_grad, gate_wgrad[None], up_wgrad[None])


def exchange_kernel(
    groups, capacity, chunks, width,
    outgoing, selection, weight_gate, weight_up, gate_pre, up_pre, hidden_grad,
    token_grad, block_rows, gate_out, up_out,
    gate_w, up_w, pre, gate_rows, up_rows, block, partial, from_core, total, from_diag,
    from_near, leaving, returned, load_sem, store_sem, local_sem, send_sem, recv_sem,
):
    e = lax.axis_index("expert")
    q = lax.axis_index("shard")
    core, x, y = q % 2, (q // 2) % 2, q // 4
    sib = q + 1 - 2 * core
    xn = q + 2 - 4 * x
    yn = q + 4 - 8 * y
    dg = xn + 4 - 8 * y
    rows = groups * capacity
    half = rows // 2
    slots = gate_rows.shape[0]
    part = slots // 4

    def pre_load(i, source):
        return pltpu.make_async_copy(source.at[0], pre.at[i], load_sem.at[2 * chunks + i])

    def weight_load(i, c, source, target):
        return pltpu.make_async_copy(
            source.at[0, pl.ds(pl.multiple_of(c * width, width), width), :],
            target.at[c], load_sem.at[2 * c + i],
        )

    def columns(c):
        return pl.ds(pl.multiple_of(c * width, width), width)

    def span(start, size):
        return pl.ds(pl.multiple_of(start, size), size)

    def held(c, start, size):
        return block.at[c, span(start, size), :]

    def chip_rows(c, device, low, size):
        return total.at[c, span(device // 2 * rows + low, size), :]

    def other(k):
        return (e + k) % groups

    def target(k):
        if k < 3:
            return (other(k + 1), q)
        if k >= 18:
            return (other(k - 17), q)
        if k in (3, 7, 12, 14, 16):
            return (e, xn)
        if k in (4, 6, 13, 15, 17):
            return (e, yn)
        return (e, sib)

    def copy(k, c):
        if k < 3:
            source = outgoing.at[other(k + 1), :, columns(c)]
            to = held(c, q * rows + e * capacity, capacity)
        elif k < 6:
            source = to = held(c, q * rows, rows)
        elif k == 6:
            source = to = held(c, xn * rows, half)
        elif k == 7:
            source = to = held(c, yn * rows + half, half)
        elif k < 11:
            source = to = held(c, (xn, yn, dg)[k - 8] * rows, rows)
        elif k == 11:
            source, to = partial.at[c, 1 - core], from_core.at[c]
        elif k == 12:
            source, to = chip_rows(c, dg, 0, half), from_diag.at[c, 0]
        elif k == 13:
            source, to = chip_rows(c, dg, half, half), from_diag.at[c, 1]
        elif k == 14:
            source, to = chip_rows(c, xn, 0, half), from_near.at[c, 0, 0]
        elif k == 15:
            source, to = chip_rows(c, yn, half, half), from_near.at[c, 1, 1]
        elif k == 16:
            source, to = chip_rows(c, xn, half, half), from_near.at[c, 0, 1]
        elif k == 17:
            source, to = chip_rows(c, yn, 0, half), from_near.at[c, 1, 0]
        else:
            source = leaving.at[c, span(other(k - 17) * capacity, capacity), :]
            to = returned.at[c, span(e * capacity, capacity), :]
        return pltpu.make_async_remote_copy(
            src_ref=source, dst_ref=to, send_sem=send_sem.at[c, k], recv_sem=recv_sem.at[c, k],
            device_id=target(k), device_id_type=MESH,
        )

    def landing(k, c):
        if k < 3:
            return held(c, q * rows + (e + groups - k - 1) % groups * capacity, capacity)
        if k < 6:
            return held(c, (xn, yn, sib)[k - 3] * rows, rows)
        if k == 6:
            return held(c, dg * rows, half)
        if k == 7:
            return held(c, dg * rows + half, half)
        if k < 11:
            return held(c, (sib + (xn, yn, dg)[k - 8] - q) * rows, rows)
        if k >= 18:
            source = (e + groups - k + 17) % groups
            return returned.at[c, span(source * capacity, capacity), :]
        return {
            11: from_core.at[c], 12: from_diag.at[c, 0], 13: from_diag.at[c, 1],
            14: from_near.at[c, 0, 0], 15: from_near.at[c, 1, 1],
            16: from_near.at[c, 0, 1], 17: from_near.at[c, 1, 0],
        }[k]

    def arrive(k, c):
        place = landing(k, c)
        pltpu.make_async_remote_copy(
            src_ref=place, dst_ref=place, send_sem=send_sem.at[c, k], recv_sem=recv_sem.at[c, k],
            device_id=target(k), device_id_type=MESH,
        ).wait_recv()

    def own_rows(c):
        return pltpu.make_async_copy(
            outgoing.at[e, :, columns(c)], held(c, q * rows + e * capacity, capacity),
            local_sem.at[c],
        )

    def rows_out(c):
        return pltpu.make_async_copy(
            block.at[c], block_rows.at[:, columns(c)], store_sem.at[c]
        )

    def grads_out(i):
        return pltpu.make_async_copy(
            (gate_rows, up_rows)[i], (gate_out, up_out)[i], store_sem.at[chunks + i]
        )

    for i, source in enumerate((gate_pre, up_pre, hidden_grad)):
        pre_load(i, source).start()

    @pl.loop(0, chunks)
    def _(c):
        weight_load(0, c, weight_gate, gate_w).start()
        weight_load(1, c, weight_up, up_w).start()
        own_rows(c).start()

    barrier = pltpu.get_barrier_semaphore()
    for device in ((other(1), q), (other(2), q), (other(3), q), (e, sib), (e, xn), (e, yn)):
        pl.semaphore_signal(barrier, inc=1, device_id=device, device_id_type=MESH)
    pl.semaphore_wait(barrier, 6)

    @pl.loop(0, chunks)
    def _(c):
        for k in (1, 0, 2):
            copy(k, c).start()

    for i, source in enumerate((gate_pre, up_pre, hidden_grad)):
        pre_load(i, source).wait()

    step_rows = 32

    @pl.loop(0, slots // step_rows)
    def _(i):
        here = span(i * step_rows, step_rows)
        gate_grad, up_grad = swiglu_grads(pre[0, here, :], pre[1, here, :], pre[2, here, :])
        gate_rows[here, :] = gate_grad
        up_rows[here, :] = up_grad

    for i in range(2):
        grads_out(i).start()

    def spread(c):
        own_rows(c).wait()
        for k in (0, 1, 2):
            arrive(k, c)
        for k in (3, 4, 5):
            copy(k, c).start()

    def forward(c):
        arrive(3, c)
        copy(6, c).start()
        copy(8, c).start()
        arrive(4, c)
        copy(7, c).start()
        copy(9, c).start()

    def far(c):
        arrive(6, c)
        arrive(7, c)
        copy(10, c).start()

    def gathered(c):
        for k in (5, 8, 9, 10):
            arrive(k, c)
        rows_out(c).start()

    def multiply(c):
        weight_load(0, c, weight_gate, gate_w).wait()
        weight_load(1, c, weight_up, up_w).wait()
        term = times_transposed(gate_rows[...], gate_w[c]) + times_transposed(up_rows[...], up_w[c])
        term = term.astype(jnp.bfloat16)
        for chip in range(slots // (2 * rows)):
            for side in range(2):
                low = (2 * chip + side) * rows
                partial[c, side, chip * rows : (chip + 1) * rows, :] = term[low : low + rows]
        copy(11, c).start()

    def pair_sum(c):
        arrive(11, c)
        both = partial[c, core].astype(jnp.float32) + from_core[c].astype(jnp.float32)
        total[c] = both.astype(jnp.bfloat16)
        for k in (12, 13, 14, 15):
            copy(k, c).start()

    def near_sum(c):
        for k, side, device, low in ((12, 0, yn, 0), (13, 1, xn, half)):
            arrive(k, c)
            place = span(device // 2 * rows + low, half)
            added = total[c, place, :].astype(jnp.float32) + from_diag[c, side].astype(jnp.float32)
            total[c, place, :] = added.astype(jnp.bfloat16)
            copy(17 if side == 0 else 16, c).start()

    def own_sum(c):
        for k in (14, 15, 16, 17):
            arrive(k, c)
        for low in range(2):
            place = span(q // 2 * rows + low * half, half)
            added = total[c, place, :].astype(jnp.float32)
            added = added + from_near[c, 0, low].astype(jnp.float32)
            added = added + from_near[c, 1, low].astype(jnp.float32)
            leaving[c, low * half : (low + 1) * half, :] = added.astype(jnp.bfloat16)
        mine = span(e * capacity, capacity)
        returned[c, mine, :] = leaving[c, mine, :]
        for k in (19, 18, 20):
            copy(k, c).start()

    def combine(c):
        for k in (18, 19, 20):
            arrive(k, c)
        token_grad[:, columns(c)] = jnp.dot(
            selection[...], returned[c], preferred_element_type=jnp.float32
        ).astype(jnp.bfloat16)

    stages = (
        (spread, 0), (forward, 1), (pair_sum, 1), (near_sum, 2), (far, 2), (own_sum, 3),
        (multiply, 0), (gathered, 3), (combine, 4),
    )

    @pl.loop(0, chunks + 4)
    def _(step):
        for stage, lag in stages:
            c = step - lag

            @pl.when(jnp.logical_and(c >= 0, c < chunks))
            def _():
                stage(c)

    @pl.loop(0, chunks)
    def _(c):
        for k in range(COPIES):
            copy(k, c).wait_send()
        rows_out(c).wait()

    for i in range(2):
        grads_out(i).wait()


def weight_grad_kernel(block_rows, gate_rows, up_rows, gate_wgrad, up_wgrad):
    left = block_rows[...]
    gate_wgrad[0] = rows_inner(left, gate_rows[...])
    up_wgrad[0] = rows_inner(left, up_rows[...])


def on_device(tokens, expert_ids, weight_gate, weight_up, gate_pre, up_pre, hidden_grad):
    groups = lax.axis_size("expert")
    shards = lax.axis_size("shard")
    token_count, model_width = tokens.shape
    slots, hidden = gate_pre.shape[1:]
    capacity = slots // (groups * shards)
    rows = groups * capacity
    chunks = CHUNKS
    width = model_width // chunks
    bf16 = jnp.bfloat16
    selection = slot_table(expert_ids, groups, capacity)
    outgoing = rows_inner(selection, tokens).astype(bf16).reshape(groups, capacity, model_width)
    in_vmem = pl.BlockSpec(memory_space=pltpu.VMEM)
    anywhere = pl.BlockSpec(memory_space=pl.ANY)
    token_grad, block_rows, gate_rows, up_rows = pl.pallas_call(
        functools.partial(exchange_kernel, groups, capacity, chunks, width),
        out_shape=(
            jax.ShapeDtypeStruct((token_count, model_width), bf16),
            jax.ShapeDtypeStruct((slots, model_width), bf16),
            jax.ShapeDtypeStruct((slots, hidden), bf16),
            jax.ShapeDtypeStruct((slots, hidden), bf16),
        ),
        in_specs=[in_vmem, in_vmem] + [anywhere] * 5,
        out_specs=(in_vmem, anywhere, anywhere, anywhere),
        scratch_shapes=[
            pltpu.VMEM((chunks, width, hidden), bf16),
            pltpu.VMEM((chunks, width, hidden), bf16),
            pltpu.VMEM((3, slots, hidden), bf16),
            pltpu.VMEM((slots, hidden), bf16),
            pltpu.VMEM((slots, hidden), bf16),
            pltpu.VMEM((chunks, slots, width), bf16),
            pltpu.VMEM((chunks, 2, slots // 2, width), bf16),
            pltpu.VMEM((chunks, slots // 2, width), bf16),
            pltpu.VMEM((chunks, slots // 2, width), bf16),
            pltpu.VMEM((chunks, 2, rows // 2, width), bf16),
            pltpu.VMEM((chunks, 2, 2, rows // 2, width), bf16),
            pltpu.VMEM((chunks, rows, width), bf16),
            pltpu.VMEM((chunks, rows, width), bf16),
            pltpu.SemaphoreType.DMA((2 * chunks + 3,)),
            pltpu.SemaphoreType.DMA((chunks + 2,)),
            pltpu.SemaphoreType.DMA((chunks,)),
            pltpu.SemaphoreType.DMA((chunks, COPIES)),
            pltpu.SemaphoreType.DMA((chunks, COPIES)),
        ],
        compiler_params=pltpu.CompilerParams(
            collective_id=0, has_side_effects=True, vmem_limit_bytes=60 * 1024 * 1024
        ),
    )(outgoing, selection, weight_gate, weight_up, gate_pre, up_pre, hidden_grad)
    tile = min(512, model_width)
    wgrad_shape = jax.ShapeDtypeStruct((1, model_width, hidden), jnp.float32)
    gate_wgrad, up_wgrad = pl.pallas_call(
        weight_grad_kernel,
        grid=(model_width // tile,),
        out_shape=(wgrad_shape, wgrad_shape),
        in_specs=[
            pl.BlockSpec((slots, tile), lambda i: (0, i)),
            pl.BlockSpec((slots, hidden), lambda i: (0, 0)),
            pl.BlockSpec((slots, hidden), lambda i: (0, 0)),
        ],
        out_specs=(
            pl.BlockSpec((1, tile, hidden), lambda i: (0, i, 0)),
            pl.BlockSpec((1, tile, hidden), lambda i: (0, i, 0)),
        ),
        compiler_params=pltpu.CompilerParams(vmem_limit_bytes=48 * 1024 * 1024),
    )(block_rows, gate_rows, up_rows)
    return (token_grad, gate_wgrad, up_wgrad)


def solution(mesh):
    placed = (
        P(("expert", "shard"), None),
        P(("expert", "shard"), None),
        P("expert", None, "shard"),
        P("expert", None, "shard"),
        P("expert", None, "shard"),
        P("expert", None, "shard"),
        P("expert", None, "shard"),
    )
    small = mesh.shape["shard"] == 8 and mesh.shape["expert"] == 4
    return jax.shard_map(
        on_device if small else on_device_general,
        mesh=mesh,
        in_specs=placed,
        out_specs=(
            P(("expert", "shard"), None),
            P("expert", None, "shard"),
            P("expert", None, "shard"),
        ),
        check_vma=False,
    )
```

```python
import functools
import jax
import jax.numpy as jnp
from jax import lax
from jax.experimental import pallas as pl
from jax.experimental.pallas import tpu as pltpu
from jax.sharding import PartitionSpec as P

MESH = pl.DeviceIdType.MESH
CHUNKS = 4
COPIES = 21


def swiglu_grads(gate_values, up_values, hidden_cotangent):
    gate_float = gate_values.astype(jnp.float32)
    up_float = up_values.astype(jnp.float32)
    cotangent = hidden_cotangent.astype(jnp.float32)
    sigmoid_gate = jax.nn.sigmoid(gate_float)
    gate_grad = (
        cotangent * up_float * sigmoid_gate * (1.0 + gate_float * (1.0 - sigmoid_gate))
    ).astype(jnp.bfloat16)
    up_grad = (cotangent * gate_float * sigmoid_gate).astype(jnp.bfloat16)
    return (gate_grad, up_grad)


def slot_table(expert_ids, groups, capacity):
    token_count = expert_ids.shape[0]
    choices_per = expert_ids.shape[1]
    labels = lax.broadcasted_iota(jnp.int32, (1, 1, groups), 2)
    one_hot = (expert_ids[:, :, None] == labels).astype(jnp.int32)
    flat_hits = one_hot.reshape(token_count * choices_per, groups)
    earlier = jnp.cumsum(flat_hits, axis=0) - flat_hits
    slot_index = jnp.sum(flat_hits * earlier, axis=1).reshape(token_count, choices_per)
    slot_labels = lax.broadcasted_iota(jnp.int32, (1, 1, 1, capacity), 3)
    slot_hits = one_hot[:, :, :, None] * (slot_index[:, :, None, None] == slot_labels).astype(
        jnp.int32
    )
    selection = jnp.sum(slot_hits, axis=1).reshape(token_count, groups * capacity)
    return selection.astype(jnp.bfloat16)


def rows_inner(left_rows, right_rows):
    return lax.dot_general(
        left_rows, right_rows, (((0,), (0,)), ((), ())), preferred_element_type=jnp.float32
    )


def times_transposed(left_rows, weights):
    return lax.dot_general(
        left_rows, weights, (((1,), (1,)), ((), ())), preferred_element_type=jnp.float32
    )


def on_device_general(tokens, expert_ids, weight_gate, weight_up, gate_pre, up_pre, hidden_grad):
    groups = lax.axis_size("expert")
    shards = lax.axis_size("shard")
    model_width = tokens.shape[1]
    capacity = gate_pre.shape[1] // (groups * shards)
    selection = slot_table(expert_ids, groups, capacity)
    outgoing = rows_inner(selection, tokens).astype(jnp.bfloat16)
    gate_grad, up_grad = swiglu_grads(gate_pre[0], up_pre[0], hidden_grad[0])
    gate_matrix = weight_gate[0]
    up_matrix = weight_up[0]
    arrived = lax.all_to_all(
        outgoing.reshape(groups, capacity, model_width),
        "expert",
        split_axis=0,
        concat_axis=0,
        tiled=True,
    )
    block_rows = lax.all_gather(
        arrived.reshape(groups * capacity, model_width), "shard", axis=0, tiled=True
    )
    gate_rows = gate_grad
    up_rows = up_grad
    gate_wgrad = rows_inner(block_rows, gate_rows)
    up_wgrad = rows_inner(block_rows, up_rows)
    gate_rows = gate_grad
    up_rows = up_grad
    summed = lax.psum_scatter(
        (times_transposed(gate_rows, gate_matrix) + times_transposed(up_rows, up_matrix)).astype(
            jnp.bfloat16
        ),
        "shard",
        scatter_dimension=0,
        tiled=True,
    )
    outbound = summed.reshape(groups, capacity, model_width)
    returned = lax.all_to_all(outbound, "expert", split_axis=0, concat_axis=0, tiled=True)
    returned = returned.reshape(groups * capacity, model_width)
    token_grad = times_transposed(selection, returned.T).astype(jnp.bfloat16)
    return (token_grad, gate_wgrad[None], up_wgrad[None])


def slot_choice(expert_ids, groups, capacity):
    token_count = expert_ids.shape[0]
    lanes = lax.broadcasted_iota(jnp.int32, (token_count, groups * capacity), 1)
    expert, slot = lanes // capacity, lanes % capacity
    named = jnp.logical_or(expert_ids[:, 0:1] == expert, expert_ids[:, 1:2] == expert)
    hits = jnp.where(named, 1.0, 0.0)
    above = lax.broadcasted_iota(jnp.int32, (token_count, token_count), 0)
    below = lax.broadcasted_iota(jnp.int32, (token_count, token_count), 1)
    before = jnp.where(below < above, 1.0, 0.0)
    earlier = jnp.dot(before, hits, preferred_element_type=jnp.float32)
    chosen = jnp.logical_and(named, earlier == slot.astype(jnp.float32))
    return jnp.where(chosen, 1.0, 0.0).astype(jnp.bfloat16)


def paced(step):
    early = jnp.where(step < 3, step, -1)
    middle = jnp.where(jnp.logical_and(step >= 4, step % 2 == 0), step // 2 + 1, early)
    return jnp.where(step > 8, step - 3, middle)


def exchange_kernel(
    groups, capacity, chunks, width,
    tokens, expert_ids, weight_gate, weight_up, gate_pre, up_pre, hidden_grad,
    returned_out, block_rows, gate_out, up_out,
    token_buf, outgoing, gate_w, up_w, pre, gate_rows, up_rows, block, partial, from_core, total, from_diag,
    from_near, leaving, returned, load_sem, store_sem, local_sem, send_sem, recv_sem,
):
    e = lax.axis_index("expert")
    q = lax.axis_index("shard")
    core, x, y = q % 2, (q // 2) % 2, q // 4
    sib = q + 1 - 2 * core
    xn = q + 2 - 4 * x
    yn = q + 4 - 8 * y
    dg = xn + 4 - 8 * y
    rows = groups * capacity
    half = rows // 2
    slots = gate_rows.shape[0]
    part = slots // 4

    def pre_load(i, source):
        return pltpu.make_async_copy(source.at[0], pre.at[i], load_sem.at[2 * chunks + i])

    def weight_load(i, c, source, target):
        return pltpu.make_async_copy(
            source.at[0, pl.ds(pl.multiple_of(c * width, width), width), :],
            target.at[c], load_sem.at[2 * c + i],
        )

    def columns(c):
        return pl.ds(pl.multiple_of(c * width, width), width)

    def span(start, size):
        return pl.ds(pl.multiple_of(start, size), size)

    def held(c, start, size):
        return block.at[c, span(start, size), :]

    def chip_rows(c, device, low, size):
        return total.at[c, span(device // 2 * rows + low, size), :]

    def other(k):
        return (e + k) % groups

    def target(k):
        if k < 3:
            return (other(k + 1), q)
        if k >= 18:
            return (other(k - 17), q)
        if k in (3, 7, 12, 14, 16):
            return (e, xn)
        if k in (4, 6, 13, 15, 17):
            return (e, yn)
        return (e, sib)

    def copy(k, c):
        if k < 3:
            source = outgoing.at[other(k + 1), :, columns(c)]
            to = held(c, q * rows + e * capacity, capacity)
        elif k < 6:
            source = to = held(c, q * rows, rows)
        elif k == 6:
            source = to = held(c, xn * rows, half)
        elif k == 7:
            source = to = held(c, yn * rows + half, half)
        elif k < 11:
            source = to = held(c, (xn, yn, dg)[k - 8] * rows, rows)
        elif k == 11:
            source, to = partial.at[c, 1 - core], from_core.at[c]
        elif k == 12:
            source, to = chip_rows(c, dg, 0, half), from_diag.at[c, 0]
        elif k == 13:
            source, to = chip_rows(c, dg, half, half), from_diag.at[c, 1]
        elif k == 14:
            source, to = chip_rows(c, xn, 0, half), from_near.at[c, 0, 0]
        elif k == 15:
            source, to = chip_rows(c, yn, half, half), from_near.at[c, 1, 1]
        elif k == 16:
            source, to = chip_rows(c, xn, half, half), from_near.at[c, 0, 1]
        elif k == 17:
            source, to = chip_rows(c, yn, 0, half), from_near.at[c, 1, 0]
        else:
            source = leaving.at[c, span(other(k - 17) * capacity, capacity), :]
            to = returned.at[c, span(e * capacity, capacity), :]
        return pltpu.make_async_remote_copy(
            src_ref=source, dst_ref=to, send_sem=send_sem.at[c, k], recv_sem=recv_sem.at[c, k],
            device_id=target(k), device_id_type=MESH,
        )

    def landing(k, c):
        if k < 3:
            return held(c, q * rows + (e + groups - k - 1) % groups * capacity, capacity)
        if k < 6:
            return held(c, (xn, yn, sib)[k - 3] * rows, rows)
        if k == 6:
            return held(c, dg * rows, half)
        if k == 7:
            return held(c, dg * rows + half, half)
        if k < 11:
            return held(c, (sib + (xn, yn, dg)[k - 8] - q) * rows, rows)
        if k >= 18:
            source = (e + groups - k + 17) % groups
            return returned.at[c, span(source * capacity, capacity), :]
        return {
            11: from_core.at[c], 12: from_diag.at[c, 0], 13: from_diag.at[c, 1],
            14: from_near.at[c, 0, 0], 15: from_near.at[c, 1, 1],
            16: from_near.at[c, 0, 1], 17: from_near.at[c, 1, 0],
        }[k]

    def arrive(k, c):
        place = landing(k, c)
        pltpu.make_async_remote_copy(
            src_ref=place, dst_ref=place, send_sem=send_sem.at[c, k], recv_sem=recv_sem.at[c, k],
            device_id=target(k), device_id_type=MESH,
        ).wait_recv()

    def own_rows(c):
        return pltpu.make_async_copy(
            outgoing.at[e, :, columns(c)], held(c, q * rows + e * capacity, capacity),
            local_sem.at[c],
        )

    def rows_out(c):
        return pltpu.make_async_copy(
            block.at[c], block_rows.at[:, columns(c)], store_sem.at[c]
        )

    def returns_out(c):
        return pltpu.make_async_copy(
            returned.at[c], returned_out.at[:, columns(c)], store_sem.at[chunks + 2 + c]
        )

    def grads_out(i):
        return pltpu.make_async_copy(
            (gate_rows, up_rows)[i], (gate_out, up_out)[i], store_sem.at[chunks + i]
        )

    token_load = pltpu.make_async_copy(tokens, token_buf, load_sem.at[2 * chunks + 3])
    token_load.start()
    for i, source in enumerate((gate_pre, up_pre, hidden_grad)):
        pre_load(i, source).start()

    @pl.loop(0, chunks)
    def _(c):
        weight_load(0, c, weight_gate, gate_w).start()
        weight_load(1, c, weight_up, up_w).start()

    barrier = pltpu.get_barrier_semaphore()
    for device in ((other(1), q), (other(2), q), (other(3), q), (e, sib), (e, xn), (e, yn)):
        pl.semaphore_signal(barrier, inc=1, device_id=device, device_id_type=MESH)
    selection = slot_choice(expert_ids[...], groups, capacity)
    token_load.wait()
    for c in range(chunks):
        here = slice(c * width, (c + 1) * width)
        picked = rows_inner(selection, token_buf[:, here]).astype(jnp.bfloat16)
        for group in range(groups):
            outgoing[group, :, here] = picked[group * capacity : (group + 1) * capacity]
    pl.semaphore_wait(barrier, 6)

    @pl.loop(0, chunks)
    def _(c):
        own_rows(c).start()
        for k in (1, 0, 2):
            copy(k, c).start()

    for i, source in enumerate((gate_pre, up_pre, hidden_grad)):
        pre_load(i, source).wait()

    step_rows = 32

    @pl.loop(0, slots // step_rows)
    def _(i):
        here = span(i * step_rows, step_rows)
        gate_grad, up_grad = swiglu_grads(pre[0, here, :], pre[1, here, :], pre[2, here, :])
        gate_rows[here, :] = gate_grad
        up_rows[here, :] = up_grad

    for i in range(2):
        grads_out(i).start()

    def spread(c):
        own_rows(c).wait()
        for k in (0, 1, 2):
            arrive(k, c)
        for k in (3, 4, 5):
            copy(k, c).start()

    def forward(c):
        arrive(3, c)
        copy(6, c).start()
        copy(8, c).start()
        arrive(4, c)
        copy(7, c).start()
        copy(9, c).start()

    def far(c):
        arrive(6, c)
        arrive(7, c)
        copy(10, c).start()

    def gathered(c):
        for k in (5, 8, 9, 10):
            arrive(k, c)
        rows_out(c).start()

    def multiply(c):
        weight_load(0, c, weight_gate, gate_w).wait()
        weight_load(1, c, weight_up, up_w).wait()
        term = times_transposed(gate_rows[...], gate_w[c]) + times_transposed(up_rows[...], up_w[c])
        term = term.astype(jnp.bfloat16)
        for chip in range(slots // (2 * rows)):
            for side in range(2):
                low = (2 * chip + side) * rows
                partial[c, side, chip * rows : (chip + 1) * rows, :] = term[low : low + rows]
        copy(11, c).start()

    def pair_sum(c):
        arrive(11, c)
        both = partial[c, core].astype(jnp.float32) + from_core[c].astype(jnp.float32)
        total[c] = both.astype(jnp.bfloat16)
        for k in (12, 13, 14, 15):
            copy(k, c).start()

    def near_sum(c):
        for k, side, device, low in ((12, 0, yn, 0), (13, 1, xn, half)):
            arrive(k, c)
            place = span(device // 2 * rows + low, half)
            added = total[c, place, :].astype(jnp.float32) + from_diag[c, side].astype(jnp.float32)
            total[c, place, :] = added.astype(jnp.bfloat16)
            copy(17 if side == 0 else 16, c).start()

    def own_sum(c):
        for k in (14, 15, 16, 17):
            arrive(k, c)
        for low in range(2):
            place = span(q // 2 * rows + low * half, half)
            added = total[c, place, :].astype(jnp.float32)
            added = added + from_near[c, 0, low].astype(jnp.float32)
            added = added + from_near[c, 1, low].astype(jnp.float32)
            leaving[c, low * half : (low + 1) * half, :] = added.astype(jnp.bfloat16)
        mine = span(e * capacity, capacity)
        returned[c, mine, :] = leaving[c, mine, :]
        for k in (19, 18, 20):
            copy(k, c).start()

    def combine(c):
        for k in (18, 19, 20):
            arrive(k, c)
        returns_out(c).start()

    stages = (
        (spread, 0, paced), (forward, 1, paced), (pair_sum, 1, None), (near_sum, 2, None),
        (far, 2, paced), (own_sum, 3, None), (multiply, 0, None), (gathered, 3, paced),
        (combine, 4, None),
    )

    @pl.loop(0, chunks + 4)
    def _(step):
        for stage, lag, pace in stages:
            c = step - lag

            @pl.when(jnp.logical_and(c >= 0, c < chunks))
            def _():
                stage(c)

    @pl.loop(0, chunks)
    def _(c):
        for k in range(COPIES):
            copy(k, c).wait_send()
        rows_out(c).wait()
        returns_out(c).wait()

    for i in range(2):
        grads_out(i).wait()


def weight_grad_kernel(
    groups, capacity, expert_ids, returned, block_rows, gate_rows, up_rows,
    token_grad, gate_wgrad, up_wgrad, selection,
):
    @pl.when(pl.program_id(0) == 0)
    def _():
        selection[...] = slot_choice(expert_ids[...], groups, capacity)

    left = block_rows[...]
    gate_wgrad[0] = rows_inner(left, gate_rows[...])
    up_wgrad[0] = rows_inner(left, up_rows[...])
    token_grad[...] = jnp.dot(
        selection[...], returned[...], preferred_element_type=jnp.float32
    ).astype(jnp.bfloat16)


def on_device(tokens, expert_ids, weight_gate, weight_up, gate_pre, up_pre, hidden_grad):
    groups = lax.axis_size("expert")
    shards = lax.axis_size("shard")
    token_count, model_width = tokens.shape
    slots, hidden = gate_pre.shape[1:]
    capacity = slots // (groups * shards)
    rows = groups * capacity
    chunks = CHUNKS
    width = model_width // chunks
    bf16 = jnp.bfloat16
    in_vmem = pl.BlockSpec(memory_space=pltpu.VMEM)
    anywhere = pl.BlockSpec(memory_space=pl.ANY)
    returned, block_rows, gate_rows, up_rows = pl.pallas_call(
        functools.partial(exchange_kernel, groups, capacity, chunks, width),
        out_shape=(
            jax.ShapeDtypeStruct((rows, model_width), bf16),
            jax.ShapeDtypeStruct((slots, model_width), bf16),
            jax.ShapeDtypeStruct((slots, hidden), bf16),
            jax.ShapeDtypeStruct((slots, hidden), bf16),
        ),
        in_specs=[anywhere, in_vmem] + [anywhere] * 5,
        out_specs=(anywhere, anywhere, anywhere, anywhere),
        scratch_shapes=[
            pltpu.VMEM((token_count, model_width), bf16),
            pltpu.VMEM((groups, capacity, model_width), bf16),
            pltpu.VMEM((chunks, width, hidden), bf16),
            pltpu.VMEM((chunks, width, hidden), bf16),
            pltpu.VMEM((3, slots, hidden), bf16),
            pltpu.VMEM((slots, hidden), bf16),
            pltpu.VMEM((slots, hidden), bf16),
            pltpu.VMEM((chunks, slots, width), bf16),
            pltpu.VMEM((chunks, 2, slots // 2, width), bf16),
            pltpu.VMEM((chunks, slots // 2, width), bf16),
            pltpu.VMEM((chunks, slots // 2, width), bf16),
            pltpu.VMEM((chunks, 2, rows // 2, width), bf16),
            pltpu.VMEM((chunks, 2, 2, rows // 2, width), bf16),
            pltpu.VMEM((chunks, rows, width), bf16),
            pltpu.VMEM((chunks, rows, width), bf16),
            pltpu.SemaphoreType.DMA((2 * chunks + 4,)),
            pltpu.SemaphoreType.DMA((2 * chunks + 2,)),
            pltpu.SemaphoreType.DMA((chunks,)),
            pltpu.SemaphoreType.DMA((chunks, COPIES)),
            pltpu.SemaphoreType.DMA((chunks, COPIES)),
        ],
        compiler_params=pltpu.CompilerParams(
            collective_id=0, has_side_effects=True, vmem_limit_bytes=60 * 1024 * 1024
        ),
    )(tokens, expert_ids, weight_gate, weight_up, gate_pre, up_pre, hidden_grad)
    tile = min(1024, model_width)
    wgrad_shape = jax.ShapeDtypeStruct((1, model_width, hidden), jnp.float32)
    token_grad, gate_wgrad, up_wgrad = pl.pallas_call(
        functools.partial(weight_grad_kernel, groups, capacity),
        grid=(model_width // tile,),
        out_shape=(jax.ShapeDtypeStruct((token_count, model_width), bf16), wgrad_shape, wgrad_shape),
        in_specs=[
            pl.BlockSpec(expert_ids.shape, lambda i: (0, 0)),
            pl.BlockSpec((rows, tile), lambda i: (0, i)),
            pl.BlockSpec((slots, tile), lambda i: (0, i)),
            pl.BlockSpec((slots, hidden), lambda i: (0, 0)),
            pl.BlockSpec((slots, hidden), lambda i: (0, 0)),
        ],
        out_specs=(
            pl.BlockSpec((token_count, tile), lambda i: (0, i)),
            pl.BlockSpec((1, tile, hidden), lambda i: (0, i, 0)),
            pl.BlockSpec((1, tile, hidden), lambda i: (0, i, 0)),
        ),
        scratch_shapes=[pltpu.VMEM((token_count, rows), bf16)],
        compiler_params=pltpu.CompilerParams(vmem_limit_bytes=63 * 1024 * 1024),
    )(expert_ids, returned, block_rows, gate_rows, up_rows)
    return (token_grad, gate_wgrad, up_wgrad)


def solution(mesh):
    placed = (
        P(("expert", "shard"), None),
        P(("expert", "shard"), None),
        P("expert", None, "shard"),
        P("expert", None, "shard"),
        P("expert", None, "shard"),
        P("expert", None, "shard"),
        P("expert", None, "shard"),
    )
    small = mesh.shape["shard"] == 8 and mesh.shape["expert"] == 4
    return jax.shard_map(
        on_device if small else on_device_general,
        mesh=mesh,
        in_specs=placed,
        out_specs=(
            P(("expert", "shard"), None),
            P("expert", None, "shard"),
            P("expert", None, "shard"),
        ),
        check_vma=False,
    )
```
